32 devices in a mesh: dp: 4 (over x, y), tp: 8 (over z, core).
Axes of the slice: x: 2, y: 2, z: 4, core: 2. Of those that a mesh axis runs over, the one named last changes fastest.
Arguments:
- residual: bfloat16 [512, 3072], P('dp'), parts along dimension 0
- positions: int32 [512], P('dp'), parts along dimension 0
- ln1_gain: bfloat16 [3072], replicated
- ln1_shift: bfloat16 [3072], replicated
- w_q: bfloat16 [3072, 3072], P(None, 'tp')
- w_k: bfloat16 [3072, 1024], P(None, 'tp')
- w_v: bfloat16 [3072, 1024], P(None, 'tp')
- w_o: bfloat16 [3072, 3072], P('tp')
- ln2_gain: bfloat16 [3072], replicated
- ln2_shift: bfloat16 [3072], replicated
- w_up: bfloat16 [3072, 9216], P(None, 'tp')
- w_down: bfloat16 [9216, 3072], P('tp')
- k_cache: bfloat16 [512, 512, 8, 128], P('dp', None, 'tp'), parts along dimension 0
- v_cache: bfloat16 [512, 512, 8, 128], P('dp', None, 'tp'), parts along dimension 0
Outputs:
- output 1: bfloat16 [512, 3072], P('dp'), parts along dimension 0
- output 2: bfloat16 [512, 8, 128], P('dp', 'tp'), parts along dimension 0
- output 3: bfloat16 [512, 8, 128], P('dp', 'tp'), parts along dimension 0
There are 4 independent parts. The reference program is written for one: setup_inputs(seed, part) draws one part's arguments, and reference() takes and returns one part's arrays. A program takes and returns all parts, laid end to end along the dimension named above; an argument that names none is the same for every part.
All inputs are finite; a program needn't handle non-finite values.
Results may differ from the reference program's by a relative error of at most 0.0165008.
Values are sent between devices in bfloat16 or wider.
A program may use at most 1 GiB of HBM per device.

```python
import math
import jax
import jax.numpy as jnp
from jax import lax

BATCH = 128
SEQ_MAX = 512
HIDDEN = 3072
Q_HEADS = 24
KV_HEADS = 8
HEAD_DIM = 128
FF_DIM = 9216
TP_SIZE = 8
KV_SLOTS = 8
ROPE_BASE = 10000

Q_WIDTH = Q_HEADS * HEAD_DIM
GROUP_SIZE = Q_HEADS // KV_SLOTS
COPIES = KV_SLOTS // KV_HEADS


def setup_inputs(seed: int = 0, part: int = 0) -> dict:
    base_key = jax.random.key(seed)
    shared_keys = jax.random.split(base_key, 10)
    part_keys = jax.random.split(jax.random.fold_in(base_key, part), 4)
    positions = jax.random.randint(part_keys[1], (BATCH,), 0, SEQ_MAX, jnp.int32)
    positions = positions.at[0].set(SEQ_MAX - 1).at[1].set(0)
    residual = jax.random.normal(part_keys[0], (BATCH, HIDDEN), jnp.float32)
    k_base = 2.5 * jax.random.normal(part_keys[2], (BATCH, SEQ_MAX, KV_HEADS, HEAD_DIM), jnp.float32)
    v_base = jax.random.normal(part_keys[3], (BATCH, SEQ_MAX, KV_HEADS, HEAD_DIM), jnp.float32)
    in_scale = HIDDEN ** -0.5
    w_q = jax.random.normal(shared_keys[0], (HIDDEN, Q_WIDTH), jnp.float32) * in_scale
    wk_base = jax.random.normal(shared_keys[1], (HIDDEN, KV_HEADS, HEAD_DIM), jnp.float32) * in_scale
    wv_base = jax.random.normal(shared_keys[2], (HIDDEN, KV_HEADS, HEAD_DIM), jnp.float32) * in_scale
    w_o = jax.random.normal(shared_keys[3], (Q_WIDTH, HIDDEN), jnp.float32) * Q_WIDTH ** -0.5
    w_up = jax.random.normal(shared_keys[4], (HIDDEN, FF_DIM), jnp.float32) * in_scale
    w_down = jax.random.normal(shared_keys[5], (FF_DIM, HIDDEN), jnp.float32) * FF_DIM ** -0.5
    norm_params = 0.4 * jax.random.normal(shared_keys[6], (4, HIDDEN), jnp.float32)
    return {
        'residual': residual.astype(jnp.bfloat16),
        'positions': positions,
        'ln1_gain': norm_params[0].astype(jnp.bfloat16),
        'ln1_shift': norm_params[1].astype(jnp.bfloat16),
        'w_q': w_q.astype(jnp.bfloat16),
        'w_k': jnp.repeat(wk_base, COPIES, axis=1).reshape(HIDDEN, KV_SLOTS * HEAD_DIM).astype(jnp.bfloat16),
        'w_v': jnp.repeat(wv_base, COPIES, axis=1).reshape(HIDDEN, KV_SLOTS * HEAD_DIM).astype(jnp.bfloat16),
        'w_o': w_o.astype(jnp.bfloat16),
        'ln2_gain': norm_params[2].astype(jnp.bfloat16),
        'ln2_shift': norm_params[3].astype(jnp.bfloat16),
        'w_up': w_up.astype(jnp.bfloat16),
        'w_down': w_down.astype(jnp.bfloat16),
        'k_cache': jnp.repeat(k_base, COPIES, axis=2).astype(jnp.bfloat16),
        'v_cache': jnp.repeat(v_base, COPIES, axis=2).astype(jnp.bfloat16),
    }


def layer_norm_1p(row_block, gain_vec, shift_vec):
    block32 = row_block.astype(jnp.float32)
    row_mean = jnp.mean(block32, axis=-1, keepdims=True)
    centered = block32 - row_mean
    row_var = jnp.mean(centered * centered, axis=-1, keepdims=True)
    normed = centered * lax.rsqrt(row_var + 1e-5)
    scaled = normed * (1.0 + gain_vec.astype(jnp.float32)) + shift_vec.astype(jnp.float32)
    return scaled.astype(jnp.bfloat16)


def rotate_first_half(head_vecs, positions):
    rot_dim = HEAD_DIM // 2
    half_rot = rot_dim // 2
    inv_freq = jnp.power(float(ROPE_BASE), -2.0 * jnp.arange(half_rot, dtype=jnp.float32) / rot_dim)
    angles = positions.astype(jnp.float32)[:, None] * inv_freq[None, :]
    cos_table = jnp.cos(angles)[:, None, :]
    sin_table = jnp.sin(angles)[:, None, :]
    vecs32 = head_vecs.astype(jnp.float32)
    first_half = vecs32[..., :half_rot]
    second_half = vecs32[..., half_rot:rot_dim]
    turned = jnp.concatenate([first_half * cos_table - second_half * sin_table, second_half * cos_table + first_half * sin_table, vecs32[..., rot_dim:]], axis=-1)
    return turned.astype(jnp.bfloat16)


def attend_row(row_items):
    q_row, k_row, v_row, k_old, v_old, where_at = row_items
    seq_index = jnp.arange(SEQ_MAX)
    is_new = (seq_index == where_at)[:, None, None]
    keys_all = jnp.where(is_new, k_row[None], k_old)
    vals_all = jnp.where(is_new, v_row[None], v_old)
    q_groups = q_row.reshape(KV_SLOTS, GROUP_SIZE, HEAD_DIM).astype(jnp.float32)
    scores = jnp.einsum('kgd,skd->kgs', q_groups, keys_all.astype(jnp.float32)) / math.sqrt(HEAD_DIM)
    scores = jnp.where((seq_index <= where_at)[None, None, :], scores, -jnp.inf)
    prob_map = jax.nn.softmax(scores, axis=-1).astype(jnp.bfloat16)
    context = jnp.einsum('kgs,skd->kgd', prob_map.astype(jnp.float32), vals_all.astype(jnp.float32))
    return context.astype(jnp.bfloat16).reshape(Q_WIDTH)


def grouped_sum(left_rows, right_mat):
    left_groups = jnp.swapaxes(left_rows.reshape(BATCH, TP_SIZE, -1), 0, 1)
    right_groups = right_mat.reshape(TP_SIZE, -1, HIDDEN)

    def add_group(running, operands):
        group_part = jnp.dot(operands[0], operands[1], preferred_element_type=jnp.float32).astype(jnp.bfloat16)
        return running + group_part.astype(jnp.float32), None

    summed, unused = lax.scan(add_group, jnp.zeros((BATCH, HIDDEN), jnp.float32), (left_groups, right_groups))
    return summed.astype(jnp.bfloat16)


def reference(residual, positions, ln1_gain, ln1_shift, w_q, w_k, w_v, w_o, ln2_gain, ln2_shift, w_up, w_down, k_cache, v_cache):
    normed = layer_norm_1p(residual, ln1_gain, ln1_shift)
    q_proj = jnp.dot(normed, w_q, preferred_element_type=jnp.float32).astype(jnp.bfloat16)
    k_proj = jnp.dot(normed, w_k, preferred_element_type=jnp.float32).astype(jnp.bfloat16)
    v_proj = jnp.dot(normed, w_v, preferred_element_type=jnp.float32).astype(jnp.bfloat16)
    q_rot = rotate_first_half(q_proj.reshape(BATCH, Q_HEADS, HEAD_DIM), positions)
    k_rot = rotate_first_half(k_proj.reshape(BATCH, KV_SLOTS, HEAD_DIM), positions)
    v_heads = v_proj.reshape(BATCH, KV_SLOTS, HEAD_DIM)
    context = lax.map(attend_row, (q_rot, k_rot, v_heads, k_cache, v_cache, positions))
    attn_sum = grouped_sum(context, w_o)
    after_attn = (residual.astype(jnp.float32) + attn_sum.astype(jnp.float32)).astype(jnp.bfloat16)
    normed_mid = layer_norm_1p(after_attn, ln2_gain, ln2_shift)
    up_proj = jnp.dot(normed_mid, w_up, preferred_element_type=jnp.float32)
    activated = jnp.square(jnp.maximum(up_proj, 0.0)).astype(jnp.bfloat16)
    mlp_sum = grouped_sum(activated, w_down)
    layer_out = (after_attn.astype(jnp.float32) + mlp_sum.astype(jnp.float32)).astype(jnp.bfloat16)
    return (layer_out, k_rot, v_heads)
```

```python
import math
import jax
import jax.numpy as jnp
from jax import lax
from jax.experimental import pallas as pl
from jax.experimental.pallas import tpu as pltpu
from jax.sharding import PartitionSpec as P

LN_EPS = 1e-5
ROPE_BASE = 10000.0


def layer_norm_1p(row_block, gain_vec, shift_vec):
    block32 = row_block.astype(jnp.float32)
    row_mean = jnp.mean(block32, axis=-1, keepdims=True)
    centered = block32 - row_mean
    row_var = jnp.mean(centered * centered, axis=-1, keepdims=True)
    normed = centered * lax.rsqrt(row_var + LN_EPS)
    scaled = normed * (1.0 + gain_vec.astype(jnp.float32)) + shift_vec.astype(jnp.float32)
    return scaled.astype(jnp.bfloat16)


def rotate_first_half(head_vecs, positions):
    head_dim = head_vecs.shape[-1]
    rot_dim = head_dim // 2
    half_rot = rot_dim // 2
    inv_freq = jnp.power(ROPE_BASE, -2.0 * jnp.arange(half_rot, dtype=jnp.float32) / rot_dim)
    angles = positions.astype(jnp.float32)[:, None] * inv_freq[None, :]
    table_shape = (head_vecs.shape[0],) + (1,) * (head_vecs.ndim - 2) + (half_rot,)
    cos_table = jnp.cos(angles).reshape(table_shape)
    sin_table = jnp.sin(angles).reshape(table_shape)
    vecs32 = head_vecs.astype(jnp.float32)
    first_half = vecs32[..., :half_rot]
    second_half = vecs32[..., half_rot:rot_dim]
    turned = jnp.concatenate([first_half * cos_table - second_half * sin_table, second_half * cos_table + first_half * sin_table, vecs32[..., rot_dim:]], axis=-1)
    return turned.astype(jnp.bfloat16)


def attend(q_rot, k_rot, v_heads, k_cache, v_cache, positions):
    row_count = k_cache.shape[0]
    seq_max = k_cache.shape[1]
    score_scale = 1.0 / math.sqrt(k_cache.shape[3])
    old_scores = jnp.einsum('rkgd,rskd->rkgs', q_rot, k_cache, preferred_element_type=jnp.float32)
    new_scores = jnp.einsum('rkgd,rkd->rkg', q_rot, k_rot, preferred_element_type=jnp.float32)
    seq_index = jnp.arange(seq_max)[None, :]
    at_pos = (seq_index == positions[:, None])[:, None, None, :]
    valid_mask = (seq_index <= positions[:, None])[:, None, None, :]
    scores = jnp.where(at_pos, new_scores[..., None], old_scores) * score_scale
    scores = jnp.where(valid_mask, scores, -jnp.inf)
    prob_map = jax.nn.softmax(scores, axis=-1).astype(jnp.bfloat16)
    zero_bf = jnp.zeros((), jnp.bfloat16)
    old_probs = jnp.where(at_pos, zero_bf, prob_map)
    new_prob = jnp.sum(jnp.where(at_pos, prob_map, zero_bf).astype(jnp.float32), axis=-1)
    context = jnp.einsum('rkgs,rskd->rkgd', old_probs, v_cache, preferred_element_type=jnp.float32)
    context = context + new_prob[..., None] * v_heads.astype(jnp.float32)[:, :, None, :]
    return context.astype(jnp.bfloat16).reshape(row_count, -1)


MESH_ID = pl.DeviceIdType.MESH
ROWS = 128
OWN = 64
MSG = 4
MROWS = 16
COLS = 3072
CSPLIT = 2
U1 = MSG * CSPLIT
CW1 = COLS // CSPLIT
U2 = 12
CW2 = COLS // U2
SKEW1 = 3
SKEW2 = 4


def tail_kernel(part_ref, res_ref, gain_ref, shift_ref, wup_hbm, wdn_hbm, out_hbm,
                wup, wdn, d1, l1, c1, t1, x1, h2, act, p2, d2, l2, c2, t2, obuf,
                w_sem, sd1, rd1, sl1, rl1, rc1, shp, rhp, she, rhe,
                sd2, rd2, sl2, rl2, rc2, sop, rop, soe, roe, o_sem):
    f32 = jnp.float32
    bf16 = jnp.bfloat16
    tp = lax.axis_index('tp')
    core = lax.rem(tp, 2)
    z = lax.div(tp, 2)
    other = 1 - core
    partner = tp + 1 - 2 * core
    line = tp + 2 - 4 * lax.rem(z, 2)
    cross = (3 - z) * 2 + core
    mid = jnp.logical_or(z == 1, z == 2)
    edge = jnp.logical_not(mid)

    load_up = pltpu.make_async_copy(wup_hbm, wup, w_sem.at[0])
    load_dn = pltpu.make_async_copy(wdn_hbm, wdn, w_sem.at[1])
    load_up.start()
    load_dn.start()

    barrier = pltpu.get_barrier_semaphore()
    pl.semaphore_signal(barrier, inc=1, device_id={'tp': partner}, device_id_type=MESH_ID)
    pl.semaphore_signal(barrier, inc=1, device_id={'tp': line}, device_id_type=MESH_ID)

    @pl.when(mid)
    def _():
        pl.semaphore_signal(barrier, inc=1, device_id={'tp': cross}, device_id_type=MESH_ID)
        pl.semaphore_wait(barrier, 3)

    @pl.when(edge)
    def _():
        pl.semaphore_wait(barrier, 2)

    def send(src, dst, ssem, rsem, dev):
        return pltpu.make_async_remote_copy(
            src_ref=src, dst_ref=dst, send_sem=ssem, recv_sem=rsem,
            device_id={'tp': dev}, device_id_type=MESH_ID)

    def cut1(u):
        return u // CSPLIT, pl.ds((u % CSPLIT) * CW1, CW1)

    def rows_of(half, m):
        return pl.ds(pl.multiple_of(half * OWN + m * MROWS, MROWS), MROWS)

    def give1(u):
        m, cs = cut1(u)
        return send(part_ref.at[rows_of(other, m), cs], d1.at[m, :, cs], sd1.at[u], rd1.at[u], partner)

    def line1(u):
        m, cs = cut1(u)
        return send(t1.at[m, :, cs], l1.at[m, :, cs], sl1.at[u], rl1.at[u], line)

    def cross1(u):
        m, cs = cut1(u)
        return send(t1.at[m, :, cs], c1.at[m, :, cs], sl1.at[u], rc1.at[u], cross)

    def share_h(m):
        return send(h2.at[core, m], h2.at[core, m], shp.at[m], rhp.at[m], partner)

    def push_h(m):
        return send(h2.at[core, m], h2.at[core, m], she.at[m], rhe.at[m], line)

    for u in range(U1):
        give1(u).start()

    def pair1(u):
        m, cs = cut1(u)
        give1(u).wait_recv()
        return part_ref[rows_of(core, m), cs].astype(f32) + d1[m, :, cs].astype(f32)

    def mid_add1(u):
        m, cs = cut1(u)
        pair = pair1(u)
        line1(u).wait_recv()
        t1[m, :, cs] = (pair + l1[m, :, cs].astype(f32)).astype(bf16)
        cross1(u).start()

    def mid_total1(u):
        m, cs = cut1(u)
        cross1(u).wait_recv()
        total = (t1[m, :, cs].astype(f32) + c1[m, :, cs].astype(f32)).astype(bf16)
        x1[m, :, cs] = (res_ref[rows_of(core, m), cs].astype(f32) + total.astype(f32)).astype(bf16)
        if u % CSPLIT == CSPLIT - 1:
            blk = x1[m].astype(f32)
            mean = jnp.mean(blk, axis=-1, keepdims=True)
            cent = blk - mean
            var = jnp.mean(cent * cent, axis=-1, keepdims=True)
            nrm = cent * lax.rsqrt(var + LN_EPS)
            h2[core, m] = (nrm * (1.0 + gain_ref[...].astype(f32)) + shift_ref[...].astype(f32)).astype(bf16)
            push_h(m).start()
            share_h(m).start()

    @pl.when(mid)
    def _():
        for s in range(U1 + SKEW1):
            if s < U1:
                mid_add1(s)
            if s >= SKEW1:
                mid_total1(s - SKEW1)

    @pl.when(edge)
    def _():
        for u in range(U1):
            m, cs = cut1(u)
            t1[m, :, cs] = pair1(u).astype(bf16)
            line1(u).start()
        for m in range(MSG):
            push_h(m).wait_recv()
            share_h(m).start()

    for m in range(MSG):
        share_h(m).wait_recv()

    load_up.wait()
    nb = 384
    hmat = h2[...].reshape(ROWS, COLS)
    for n in range(wup.shape[1] // nb):
        up = jnp.dot(hmat, wup[:, n * nb:(n + 1) * nb], preferred_element_type=f32)
        act[:, n * nb:(n + 1) * nb] = jnp.square(jnp.maximum(up, 0.0)).astype(bf16)
    load_dn.wait()

    def give2(u):
        return send(p2.at[u, other], d2.at[u], sd2.at[u], rd2.at[u], partner)

    def line2(u):
        return send(t2.at[u], l2.at[u], sl2.at[u], rl2.at[u], line)

    def cross2(u):
        return send(t2.at[u], c2.at[u], sl2.at[u], rc2.at[u], cross)

    def share_o(u):
        return send(obuf.at[u, core], obuf.at[u, core], sop.at[u], rop.at[u], partner)

    def push_o(u):
        return send(obuf.at[u, core], obuf.at[u, core], soe.at[u], roe.at[u], line)

    def put_o(u, half):
        return pltpu.make_async_copy(
            obuf.at[u, half],
            out_hbm.at[pl.ds(pl.multiple_of(half * OWN, OWN), OWN), pl.ds(u * CW2, CW2)],
            o_sem.at[u, half])

    def down(u):
        dn = jnp.dot(act[...], wdn[:, u * CW2:(u + 1) * CW2], preferred_element_type=f32)
        p2[u] = dn.astype(bf16).reshape(2, OWN, CW2)
        give2(u).start()

    def pair2(u):
        give2(u).wait_recv()
        return p2[u, core].astype(f32) + d2[u].astype(f32)

    def mid_add2(u):
        pair = pair2(u)
        line2(u).wait_recv()
        t2[u] = (pair + l2[u].astype(f32)).astype(bf16)
        cross2(u).start()

    def mid_total2(u):
        cross2(u).wait_recv()
        total = (t2[u].astype(f32) + c2[u].astype(f32)).astype(bf16)
        own = x1[:, :, u * CW2:(u + 1) * CW2].reshape(OWN, CW2)
        obuf[u, core] = (own.astype(f32) + total.astype(f32)).astype(bf16)
        push_o(u).start()
        share_o(u).start()
        put_o(u, core).start()

    @pl.when(mid)
    def _():
        down(0)
        down(1)
        for s in range(U2 + SKEW2):
            if s + 2 < U2:
                down(s + 2)
            if s < U2:
                mid_add2(s)
            if s >= SKEW2:
                mid_total2(s - SKEW2)

    @pl.when(edge)
    def _():
        down(0)
        down(1)
        for u in range(U2):
            if u + 2 < U2:
                down(u + 2)
            t2[u] = pair2(u).astype(bf16)
            line2(u).start()
        for u in range(U2):
            push_o(u).wait_recv()
            share_o(u).start()
            put_o(u, core).start()

    for u in range(U2):
        share_o(u).wait_recv()
        put_o(u, other).start()

    for u in range(U1):
        give1(u).wait_send()
        line1(u).wait_send()
    for m in range(MSG):
        share_h(m).wait_send()
    for u in range(U2):
        give2(u).wait_send()
        line2(u).wait_send()
        share_o(u).wait_send()
        put_o(u, core).wait()
        put_o(u, other).wait()

    @pl.when(mid)
    def _():
        for m in range(MSG):
            push_h(m).wait_send()
        for u in range(U2):
            push_o(u).wait_send()


def tail_call(part, residual, gain, shift, w_up, w_down):
    bf16 = jnp.bfloat16
    ff = w_up.shape[1]
    vm = pl.BlockSpec(memory_space=pltpu.VMEM)
    hb = pl.BlockSpec(memory_space=pl.ANY)
    dma = pltpu.SemaphoreType.DMA
    return pl.pallas_call(
        tail_kernel,
        name='tail',
        out_shape=jax.ShapeDtypeStruct((ROWS, COLS), bf16),
        in_specs=[vm, vm, vm, vm, hb, hb],
        out_specs=hb,
        scratch_shapes=[
            pltpu.VMEM((COLS, ff), bf16), pltpu.VMEM((ff, COLS), bf16),
            pltpu.VMEM((MSG, MROWS, COLS), bf16), pltpu.VMEM((MSG, MROWS, COLS), bf16),
            pltpu.VMEM((MSG, MROWS, COLS), bf16), pltpu.VMEM((MSG, MROWS, COLS), bf16),
            pltpu.VMEM((MSG, MROWS, COLS), bf16),
            pltpu.VMEM((2, MSG, MROWS, COLS), bf16),
            pltpu.VMEM((ROWS, ff), bf16),
            pltpu.VMEM((U2, 2, OWN, CW2), bf16),
            pltpu.VMEM((U2, OWN, CW2), bf16), pltpu.VMEM((U2, OWN, CW2), bf16),
            pltpu.VMEM((U2, OWN, CW2), bf16), pltpu.VMEM((U2, OWN, CW2), bf16),
            pltpu.VMEM((U2, 2, OWN, CW2), bf16),
            dma((2,)),
            dma((U1,)), dma((U1,)), dma((U1,)), dma((U1,)), dma((U1,)),
            dma((MSG,)), dma((MSG,)), dma((MSG,)), dma((MSG,)),
            dma((U2,)), dma((U2,)), dma((U2,)), dma((U2,)), dma((U2,)),
            dma((U2,)), dma((U2,)), dma((U2,)), dma((U2,)),
            dma((U2, 2)),
        ],
        compiler_params=pltpu.CompilerParams(collective_id=0, has_side_effects=True, vmem_limit_bytes=50 * 1024 * 1024),
    )(part, residual, gain, shift, w_up, w_down)


def solution(mesh):
    row_spec = P('dp', None)
    whole_spec = P()
    col_spec = P(None, 'tp')
    wrow_spec = P('tp', None)
    cache_spec = P('dp', None, 'tp', None)
    new_spec = P('dp', 'tp', None)
    arg_specs = (row_spec, P('dp'), whole_spec, whole_spec, col_spec, col_spec, col_spec, wrow_spec, whole_spec, whole_spec, col_spec, wrow_spec, cache_spec, cache_spec)

    def local_step(residual, positions, ln1_gain, ln1_shift, w_q, w_k, w_v, w_o, ln2_gain, ln2_shift, w_up, w_down, k_cache, v_cache):
        row_count = residual.shape[0]
        slots_here = k_cache.shape[2]
        head_dim = k_cache.shape[3]
        group_size = w_q.shape[1] // (head_dim * slots_here)
        normed = layer_norm_1p(residual, ln1_gain, ln1_shift)
        q_proj = jnp.dot(normed, w_q, preferred_element_type=jnp.float32).astype(jnp.bfloat16)
        k_proj = jnp.dot(normed, w_k, preferred_element_type=jnp.float32).astype(jnp.bfloat16)
        v_proj = jnp.dot(normed, w_v, preferred_element_type=jnp.float32).astype(jnp.bfloat16)
        q_rot = rotate_first_half(q_proj.reshape(row_count, slots_here, group_size, head_dim), positions)
        k_rot = rotate_first_half(k_proj.reshape(row_count, slots_here, head_dim), positions)
        v_heads = v_proj.reshape(row_count, slots_here, head_dim)
        context = attend(q_rot, k_rot, v_heads, k_cache, v_cache, positions)
        attn_part = jnp.dot(context, w_o, preferred_element_type=jnp.float32).astype(jnp.bfloat16)
        layer_out = tail_call(attn_part, residual, ln2_gain[None, :], ln2_shift[None, :], w_up, w_down)
        return layer_out, k_rot, v_heads

    return jax.shard_map(local_step, mesh=mesh, in_specs=arg_specs, out_specs=(row_spec, new_spec, new_spec), check_vma=False)
```

```python
import math
import jax
import jax.numpy as jnp
from jax import lax
from jax.experimental import pallas as pl
from jax.experimental.pallas import tpu as pltpu
from jax.sharding import PartitionSpec as P

LN_EPS = 1e-5
ROPE_BASE = 10000.0


MESH_ID = pl.DeviceIdType.MESH
ROWS = 128
OWN = 64
MSG = 4
MROWS = 16
COLS = 3072
CSPLIT = 2
U1 = MSG * CSPLIT
CW1 = COLS // CSPLIT
U2 = 12
CW2 = COLS // U2
SKEW1 = 3
SKEW2 = 4


def tail_kernel(part_ref, res_ref, gain_ref, shift_ref, wup_hbm, wdn_hbm, out_hbm,
                wup, wdn, d1, l1, c1, t1, x1, h2, act, p2, d2, l2, c2, t2, obuf,
                w_sem, sd1, rd1, sl1, rl1, rc1, shp, rhp, she, rhe,
                sd2, rd2, sl2, rl2, rc2, sop, rop, soe, roe, o_sem):
    f32 = jnp.float32
    bf16 = jnp.bfloat16
    tp = lax.axis_index('tp')
    core = lax.rem(tp, 2)
    z = lax.div(tp, 2)
    other = 1 - core
    partner = tp + 1 - 2 * core
    line = tp + 2 - 4 * lax.rem(z, 2)
    cross = (3 - z) * 2 + core
    mid = jnp.logical_or(z == 1, z == 2)
    edge = jnp.logical_not(mid)

    load_up = pltpu.make_async_copy(wup_hbm, wup, w_sem.at[0])
    load_dn = pltpu.make_async_copy(wdn_hbm, wdn, w_sem.at[1])
    load_up.start()
    load_dn.start()

    barrier = pltpu.get_barrier_semaphore()
    pl.semaphore_signal(barrier, inc=1, device_id={'tp': partner}, device_id_type=MESH_ID)
    pl.semaphore_signal(barrier, inc=1, device_id={'tp': line}, device_id_type=MESH_ID)

    @pl.when(mid)
    def _():
        pl.semaphore_signal(barrier, inc=1, device_id={'tp': cross}, device_id_type=MESH_ID)
        pl.semaphore_wait(barrier, 3)

    @pl.when(edge)
    def _():
        pl.semaphore_wait(barrier, 2)

    def send(src, dst, ssem, rsem, dev):
        return pltpu.make_async_remote_copy(
            src_ref=src, dst_ref=dst, send_sem=ssem, recv_sem=rsem,
            device_id={'tp': dev}, device_id_type=MESH_ID)

    def cut1(u):
        return u // CSPLIT, pl.ds((u % CSPLIT) * CW1, CW1)

    def rows_of(half, m):
        return pl.ds(pl.multiple_of(half * OWN + m * MROWS, MROWS), MROWS)

    def give1(u):
        m, cs = cut1(u)
        return send(part_ref.at[rows_of(other, m), cs], d1.at[m, :, cs], sd1.at[u], rd1.at[u], partner)

    def line1(u):
        m, cs = cut1(u)
        return send(t1.at[m, :, cs], l1.at[m, :, cs], sl1.at[u], rl1.at[u], line)

    def cross1(u):
        m, cs = cut1(u)
        return send(t1.at[m, :, cs], c1.at[m, :, cs], sl1.at[u], rc1.at[u], cross)

    def share_h(m):
        return send(h2.at[core, m], h2.at[core, m], shp.at[m], rhp.at[m], partner)

    def push_h(m):
        return send(h2.at[core, m], h2.at[core, m], she.at[m], rhe.at[m], line)

    for u in range(U1):
        give1(u).start()

    def pair1(u):
        m, cs = cut1(u)
        give1(u).wait_recv()
        return part_ref[rows_of(core, m), cs].astype(f32) + d1[m, :, cs].astype(f32)

    def mid_add1(u):
        m, cs = cut1(u)
        pair = pair1(u)
        line1(u).wait_recv()
        t1[m, :, cs] = (pair + l1[m, :, cs].astype(f32)).astype(bf16)
        cross1(u).start()

    def mid_total1(u):
        m, cs = cut1(u)
        cross1(u).wait_recv()
        total = (t1[m, :, cs].astype(f32) + c1[m, :, cs].astype(f32)).astype(bf16)
        x1[m, :, cs] = (res_ref[rows_of(core, m), cs].astype(f32) + total.astype(f32)).astype(bf16)
        if u % CSPLIT == CSPLIT - 1:
            blk = x1[m].astype(f32)
            mean = jnp.mean(blk, axis=-1, keepdims=True)
            cent = blk - mean
            var = jnp.mean(cent * cent, axis=-1, keepdims=True)
            nrm = cent * lax.rsqrt(var + LN_EPS)
            h2[core, m] = (nrm * (1.0 + gain_ref[...].astype(f32)) + shift_ref[...].astype(f32)).astype(bf16)
            push_h(m).start()
            share_h(m).start()

    @pl.when(mid)
    def _():
        for s in range(U1 + SKEW1):
            if s < U1:
                mid_add1(s)
            if s >= SKEW1:
                mid_total1(s - SKEW1)

    @pl.when(edge)
    def _():
        for u in range(U1):
            m, cs = cut1(u)
            t1[m, :, cs] = pair1(u).astype(bf16)
            line1(u).start()
        for m in range(MSG):
            push_h(m).wait_recv()
            share_h(m).start()

    for m in range(MSG):
        share_h(m).wait_recv()

    load_up.wait()
    nb = 384
    hmat = h2[...].reshape(ROWS, COLS)
    for n in range(wup.shape[1] // nb):
        up = jnp.dot(hmat, wup[:, n * nb:(n + 1) * nb], preferred_element_type=f32)
        act[:, n * nb:(n + 1) * nb] = jnp.square(jnp.maximum(up, 0.0)).astype(bf16)
    load_dn.wait()

    def give2(u):
        return send(p2.at[u, other], d2.at[u], sd2.at[u], rd2.at[u], partner)

    def line2(u):
        return send(t2.at[u], l2.at[u], sl2.at[u], rl2.at[u], line)

    def cross2(u):
        return send(t2.at[u], c2.at[u], sl2.at[u], rc2.at[u], cross)

    def share_o(u):
        return send(obuf.at[u, core], obuf.at[u, core], sop.at[u], rop.at[u], partner)

    def push_o(u):
        return send(obuf.at[u, core], obuf.at[u, core], soe.at[u], roe.at[u], line)

    def put_o(u, half):
        return pltpu.make_async_copy(
            obuf.at[u, half],
            out_hbm.at[pl.ds(pl.multiple_of(half * OWN, OWN), OWN), pl.ds(u * CW2, CW2)],
            o_sem.at[u, half])

    def down(u):
        dn = jnp.dot(act[...], wdn[:, u * CW2:(u + 1) * CW2], preferred_element_type=f32)
        p2[u] = dn.astype(bf16).reshape(2, OWN, CW2)
        give2(u).start()

    def pair2(u):
        give2(u).wait_recv()
        return p2[u, core].astype(f32) + d2[u].astype(f32)

    def mid_add2(u):
        pair = pair2(u)
        line2(u).wait_recv()
        t2[u] = (pair + l2[u].astype(f32)).astype(bf16)
        cross2(u).start()

    def mid_total2(u):
        cross2(u).wait_recv()
        total = (t2[u].astype(f32) + c2[u].astype(f32)).astype(bf16)
        own = x1[:, :, u * CW2:(u + 1) * CW2].reshape(OWN, CW2)
        obuf[u, core] = (own.astype(f32) + total.astype(f32)).astype(bf16)
        push_o(u).start()
        share_o(u).start()
        put_o(u, core).start()

    @pl.when(mid)
    def _():
        down(0)
        down(1)
        for s in range(U2 + SKEW2):
            if s + 2 < U2:
                down(s + 2)
            if s < U2:
                mid_add2(s)
            if s >= SKEW2:
                mid_total2(s - SKEW2)

    @pl.when(edge)
    def _():
        down(0)
        down(1)
        for u in range(U2):
            if u + 2 < U2:
                down(u + 2)
            t2[u] = pair2(u).astype(bf16)
            line2(u).start()
        for u in range(U2):
            push_o(u).wait_recv()
            share_o(u).start()
            put_o(u, core).start()

    for u in range(U2):
        share_o(u).wait_recv()
        put_o(u, other).start()

    for u in range(U1):
        give1(u).wait_send()
        line1(u).wait_send()
    for m in range(MSG):
        share_h(m).wait_send()
    for u in range(U2):
        give2(u).wait_send()
        line2(u).wait_send()
        share_o(u).wait_send()
        put_o(u, core).wait()
        put_o(u, other).wait()

    @pl.when(mid)
    def _():
        for m in range(MSG):
            push_h(m).wait_send()
        for u in range(U2):
            push_o(u).wait_send()


def tail_call(part, residual, gain, shift, w_up, w_down):
    bf16 = jnp.bfloat16
    ff = w_up.shape[1]
    vm = pl.BlockSpec(memory_space=pltpu.VMEM)
    hb = pl.BlockSpec(memory_space=pl.ANY)
    dma = pltpu.SemaphoreType.DMA
    return pl.pallas_call(
        tail_kernel,
        name='tail',
        out_shape=jax.ShapeDtypeStruct((ROWS, COLS), bf16),
        in_specs=[vm, vm, vm, vm, hb, hb],
        out_specs=hb,
        scratch_shapes=[
            pltpu.VMEM((COLS, ff), bf16), pltpu.VMEM((ff, COLS), bf16),
            pltpu.VMEM((MSG, MROWS, COLS), bf16), pltpu.VMEM((MSG, MROWS, COLS), bf16),
            pltpu.VMEM((MSG, MROWS, COLS), bf16), pltpu.VMEM((MSG, MROWS, COLS), bf16),
            pltpu.VMEM((MSG, MROWS, COLS), bf16),
            pltpu.VMEM((2, MSG, MROWS, COLS), bf16),
            pltpu.VMEM((ROWS, ff), bf16),
            pltpu.VMEM((U2, 2, OWN, CW2), bf16),
            pltpu.VMEM((U2, OWN, CW2), bf16), pltpu.VMEM((U2, OWN, CW2), bf16),
            pltpu.VMEM((U2, OWN, CW2), bf16), pltpu.VMEM((U2, OWN, CW2), bf16),
            pltpu.VMEM((U2, 2, OWN, CW2), bf16),
            dma((2,)),
            dma((U1,)), dma((U1,)), dma((U1,)), dma((U1,)), dma((U1,)),
            dma((MSG,)), dma((MSG,)), dma((MSG,)), dma((MSG,)),
            dma((U2,)), dma((U2,)), dma((U2,)), dma((U2,)), dma((U2,)),
            dma((U2,)), dma((U2,)), dma((U2,)), dma((U2,)),
            dma((U2, 2)),
        ],
        compiler_params=pltpu.CompilerParams(collective_id=0, has_side_effects=True, vmem_limit_bytes=50 * 1024 * 1024),
    )(part, residual, gain, shift, w_up, w_down)


HDIM = 128
SEQ = 512
GRP = 32
NGRP = ROWS // GRP
SUB = 8
NSUB = GRP // SUB
ROT = 64


def head_kernel(x_hbm, pos_ref, gain_ref, shift_ref, wq_hbm, wk_hbm, wv_hbm, wo_hbm, k_hbm, v_hbm,
                part_ref, knew_ref, vnew_ref,
                xs, hs, wqkv, wo, kb, vb, qs, ks, vs, ps, cs, ss,
                in_sem, w_sem, k_sem, v_sem):
    f32 = jnp.float32
    bf16 = jnp.bfloat16
    nq = wq_hbm.shape[1]

    load_x = pltpu.make_async_copy(x_hbm, xs, in_sem.at[0])
    load_q = pltpu.make_async_copy(wq_hbm, wqkv.at[:, pl.ds(0, nq)], w_sem.at[0])
    load_k = pltpu.make_async_copy(wk_hbm, wqkv.at[:, pl.ds(nq, HDIM)], w_sem.at[1])
    load_v = pltpu.make_async_copy(wv_hbm, wqkv.at[:, pl.ds(nq + HDIM, HDIM)], w_sem.at[2])
    load_o = pltpu.make_async_copy(wo_hbm, wo, in_sem.at[1])

    def key_copy(g, s):
        at = pl.ds(g * GRP + s * SUB, SUB)
        return pltpu.make_async_copy(k_hbm.at[at], kb.at[at], k_sem.at[g, s])

    def val_copy(g, s):
        at = pl.ds(g * GRP + s * SUB, SUB)
        return pltpu.make_async_copy(v_hbm.at[at], vb.at[at], v_sem.at[g, s])

    load_x.start()
    load_q.start()
    load_k.start()
    load_v.start()
    for g in range(NGRP):
        for s in range(NSUB):
            key_copy(g, s).start()
        if g == NGRP - 1:
            load_o.start()
        for s in range(NSUB):
            val_copy(g, s).start()

    lane = lax.broadcasted_iota(jnp.int32, (ROWS, HDIM), 1)
    pos_col = jnp.transpose(jnp.broadcast_to(pos_ref[...].astype(f32), (ROWS, ROWS)))
    half = ROT // 2
    pair = lax.rem(lane, half).astype(f32)
    inv = jnp.exp(pair * (-2.0 * math.log(ROPE_BASE) / ROT))
    ang = pos_col * inv
    in_rot = lane < ROT
    cos_t = jnp.where(in_rot, jnp.cos(ang), 1.0)
    sin_a = jnp.sin(ang)
    sin_t = jnp.where(in_rot, jnp.where(lane < half, -sin_a, sin_a), 0.0)

    def rotate(v):
        swap = jnp.where(lane < half, pltpu.roll(v, HDIM - half, 1), pltpu.roll(v, half, 1))
        return (v * cos_t + swap * sin_t).astype(bf16)

    load_x.wait()
    rb = 32
    gain1 = 1.0 + gain_ref[...].astype(f32)
    shift1 = shift_ref[...].astype(f32)
    for r in range(ROWS // rb):
        blk = xs[r * rb:(r + 1) * rb, :].astype(f32)
        mean = jnp.mean(blk, axis=-1, keepdims=True)
        cent = blk - mean
        var = jnp.mean(cent * cent, axis=-1, keepdims=True)
        nrm = cent * lax.rsqrt(var + LN_EPS)
        hs[r * rb:(r + 1) * rb, :] = (nrm * gain1 + shift1).astype(bf16)

    load_q.wait()
    load_k.wait()
    load_v.wait()
    qkv = jnp.dot(hs[...], wqkv[...], preferred_element_type=f32).astype(bf16).astype(f32)
    k_rot = rotate(qkv[:, nq:nq + HDIM])
    v_head = qkv[:, nq + HDIM:nq + 2 * HDIM]
    knew_ref[...] = k_rot
    vnew_ref[...] = v_head.astype(bf16)
    heads = nq // HDIM
    for g in range(4):
        at = pl.ds(g, ROWS, stride=4)
        if g < heads:
            qs[at, :] = rotate(qkv[:, g * HDIM:(g + 1) * HDIM]).astype(f32)
        else:
            qs[at, :] = jnp.zeros((ROWS, HDIM), f32)
        ks[at, :] = k_rot.astype(f32)
        vs[at, :] = v_head
        ps[at, :] = pos_col

    scale = 1.0 / math.sqrt(HDIM)
    lane_b = lax.div(lane, 4)
    row_i = lax.div(lax.broadcasted_iota(jnp.int32, (16, HDIM), 0), 4)
    step_t = lax.broadcasted_iota(jnp.int32, (SEQ, HDIM), 0)

    def group(g, carry):
        rows = pl.ds(pl.multiple_of(g * (GRP * 4), GRP * 4), GRP * 4)
        qg = qs[rows, :]
        q_t = jnp.transpose(qg)
        p_row = jnp.transpose(ps[rows, :])[0:1, :].astype(jnp.int32)
        new_col = jnp.sum(qg * ks[rows, :], axis=-1, keepdims=True)
        new_row = jnp.transpose(jnp.broadcast_to(new_col, (HDIM, HDIM)))[0:1, :]
        for s in range(NSUB):
            key_copy(g, s).wait()
            base = g * GRP + s * SUB
            left = jnp.concatenate([kb[base + i] for i in range(SUB)], axis=1)
            right = jnp.concatenate(
                [jnp.where(lane_b == s * SUB + i, q_t, 0.0).astype(bf16) for i in range(SUB)], axis=0)
            acc = jnp.dot(left, right, preferred_element_type=f32)
            if s == 0:
                ss[...] = acc
            else:
                ss[...] += acc
        is_new = step_t == p_row
        sc = jnp.where(is_new, new_row, ss[...]) * scale
        sc = jnp.where(step_t <= p_row, sc, -jnp.inf)
        top = jnp.max(sc, axis=0, keepdims=True)
        ex = jnp.exp(sc - top)
        pr = ex * (1.0 / jnp.sum(ex, axis=0, keepdims=True))
        p_new = jnp.sum(jnp.where(is_new, pr, 0.0), axis=0, keepdims=True).astype(bf16).astype(f32)
        new_w = jnp.transpose(jnp.broadcast_to(p_new, (HDIM, HDIM)))
        p_t = jnp.transpose(jnp.where(is_new, 0.0, pr)).astype(bf16)
        extra = new_w * vs[rows, :]
        for s in range(NSUB):
            val_copy(g, s).wait()
            for j in range(SUB // 4):
                base = g * GRP + s * SUB + j * 4
                at = (s * SUB + j * 4) * 4
                right = jnp.concatenate([vb[base + i] for i in range(4)], axis=1)
                mix = jnp.dot(p_t[at:at + 16, :], right, preferred_element_type=f32)
                out = extra[at:at + 16, :]
                for i in range(4):
                    out = out + jnp.where(row_i == i, mix[:, i * HDIM:(i + 1) * HDIM], 0.0)
                cs[pl.ds(pl.multiple_of(g * (GRP * 4) + at, 16), 16), :] = out
        return carry

    lax.fori_loop(0, NGRP, group, 0)

    ctx = jnp.concatenate([cs[pl.ds(g, ROWS, stride=4), :].astype(bf16) for g in range(heads)], axis=1)
    load_o.wait()
    wide = 512
    for n in range(COLS // wide):
        part_ref[:, n * wide:(n + 1) * wide] = jnp.dot(
            ctx, wo[:, n * wide:(n + 1) * wide], preferred_element_type=f32).astype(bf16)


def head_call(residual, positions, gain, shift, w_q, w_k, w_v, w_o, keys, vals):
    bf16 = jnp.bfloat16
    f32 = jnp.float32
    vm = pl.BlockSpec(memory_space=pltpu.VMEM)
    hb = pl.BlockSpec(memory_space=pl.ANY)
    dma = pltpu.SemaphoreType.DMA
    nq = w_q.shape[1]
    return pl.pallas_call(
        head_kernel,
        name='head',
        out_shape=(jax.ShapeDtypeStruct((ROWS, COLS), bf16),
                   jax.ShapeDtypeStruct((ROWS, HDIM), bf16),
                   jax.ShapeDtypeStruct((ROWS, HDIM), bf16)),
        in_specs=[hb, vm, vm, vm, hb, hb, hb, hb, hb, hb],
        out_specs=(vm, vm, vm),
        scratch_shapes=[
            pltpu.VMEM((ROWS, COLS), bf16), pltpu.VMEM((ROWS, COLS), bf16),
            pltpu.VMEM((COLS, nq + 2 * HDIM), bf16), pltpu.VMEM((nq, COLS), bf16),
            pltpu.VMEM((ROWS, SEQ, HDIM), bf16), pltpu.VMEM((ROWS, SEQ, HDIM), bf16),
            pltpu.VMEM((ROWS * 4, HDIM), f32), pltpu.VMEM((ROWS * 4, HDIM), f32),
            pltpu.VMEM((ROWS * 4, HDIM), f32), pltpu.VMEM((ROWS * 4, HDIM), f32),
            pltpu.VMEM((ROWS * 4, HDIM), f32),
            pltpu.VMEM((SEQ, HDIM), f32),
            dma((2,)), dma((3,)), dma((NGRP, NSUB)), dma((NGRP, NSUB)),
        ],
        compiler_params=pltpu.CompilerParams(vmem_limit_bytes=58 * 1024 * 1024),
    )(residual, positions, gain, shift, w_q, w_k, w_v, w_o, keys, vals)


def solution(mesh):
    row_spec = P('dp', None)
    whole_spec = P()
    col_spec = P(None, 'tp')
    wrow_spec = P('tp', None)
    cache_spec = P('dp', None, 'tp', None)
    new_spec = P('dp', 'tp', None)
    arg_specs = (row_spec, P('dp'), whole_spec, whole_spec, col_spec, col_spec, col_spec, wrow_spec, whole_spec, whole_spec, col_spec, wrow_spec, cache_spec, cache_spec)

    def local_step(residual, positions, ln1_gain, ln1_shift, w_q, w_k, w_v, w_o, ln2_gain, ln2_shift, w_up, w_down, k_cache, v_cache):
        row_count = residual.shape[0]
        keys = k_cache.reshape(row_count, k_cache.shape[1], k_cache.shape[3])
        vals = v_cache.reshape(row_count, v_cache.shape[1], v_cache.shape[3])
        attn_part, k_rot, v_head = head_call(residual, positions[None, :], ln1_gain[None, :], ln1_shift[None, :], w_q, w_k, w_v, w_o, keys, vals)
        layer_out = tail_call(attn_part, residual, ln2_gain[None, :], ln2_shift[None, :], w_up, w_down)
        return layer_out, k_rot[:, None, :], v_head[:, None, :]

    return jax.shard_map(local_step, mesh=mesh, in_specs=arg_specs, out_specs=(row_spec, new_spec, new_spec), check_vma=False)
```

```python
import math
import jax
import jax.numpy as jnp
from jax import lax
from jax.experimental import pallas as pl
from jax.experimental.pallas import tpu as pltpu
from jax.sharding import PartitionSpec as P

LN_EPS = 1e-5
ROPE_BASE = 10000.0


MESH_ID = pl.DeviceIdType.MESH
ROWS = 128
OWN = 64
MSG = 4
MROWS = 16
COLS = 3072
CSPLIT = 2
U1 = MSG * CSPLIT
CW1 = COLS // CSPLIT
U2 = 12
CW2 = COLS // U2
SKEW1 = 3
SKEW2 = 4


def tail_kernel(part_ref, res_ref, gain_ref, shift_ref, wup_hbm, wdn_hbm, out_hbm,
                wup, wdn, d1, l1, c1, t1, x1, h2, act, p2, d2, l2, c2, t2, obuf, gs,
                w_sem, sd1, rd1, sl1, rl1, rc1, shp, rhp, she, rhe,
                sd2, rd2, sl2, rl2, rc2, sop, rop, soe, roe, o_sem):
    f32 = jnp.float32
    bf16 = jnp.bfloat16
    tp = lax.axis_index('tp')
    core = lax.rem(tp, 2)
    z = lax.div(tp, 2)
    other = 1 - core
    partner = tp + 1 - 2 * core
    line = tp + 2 - 4 * lax.rem(z, 2)
    cross = (3 - z) * 2 + core
    mid = jnp.logical_or(z == 1, z == 2)
    edge = jnp.logical_not(mid)

    load_up = pltpu.make_async_copy(wup_hbm, wup, w_sem.at[0])
    load_dn = pltpu.make_async_copy(wdn_hbm, wdn, w_sem.at[1])
    load_up.start()
    load_dn.start()

    for j in range(COLS // 128):
        at = slice(j * 128, (j + 1) * 128)
        gs[0:1, at] = 1.0 + gain_ref[j:j + 1, :].astype(f32)
        gs[1:2, at] = shift_ref[j:j + 1, :].astype(f32)

    barrier = pltpu.get_barrier_semaphore()
    pl.semaphore_signal(barrier, inc=1, device_id={'tp': partner}, device_id_type=MESH_ID)
    pl.semaphore_signal(barrier, inc=1, device_id={'tp': line}, device_id_type=MESH_ID)

    @pl.when(mid)
    def _():
        pl.semaphore_signal(barrier, inc=1, device_id={'tp': cross}, device_id_type=MESH_ID)
        pl.semaphore_wait(barrier, 3)

    @pl.when(edge)
    def _():
        pl.semaphore_wait(barrier, 2)

    def send(src, dst, ssem, rsem, dev):
        return pltpu.make_async_remote_copy(
            src_ref=src, dst_ref=dst, send_sem=ssem, recv_sem=rsem,
            device_id={'tp': dev}, device_id_type=MESH_ID)

    def cut1(u):
        return u // CSPLIT, pl.ds((u % CSPLIT) * CW1, CW1)

    def rows_of(half, m):
        return pl.ds(pl.multiple_of(half * OWN + m * MROWS, MROWS), MROWS)

    def give1(u):
        m, cs = cut1(u)
        return send(part_ref.at[rows_of(other, m), cs], d1.at[m, :, cs], sd1.at[u], rd1.at[u], partner)

    def line1(u):
        m, cs = cut1(u)
        return send(t1.at[m, :, cs], l1.at[m, :, cs], sl1.at[u], rl1.at[u], line)

    def cross1(u):
        m, cs = cut1(u)
        return send(t1.at[m, :, cs], c1.at[m, :, cs], sl1.at[u], rc1.at[u], cross)

    def share_h(m):
        return send(h2.at[core, m], h2.at[core, m], shp.at[m], rhp.at[m], partner)

    def push_h(m):
        return send(h2.at[core, m], h2.at[core, m], she.at[m], rhe.at[m], line)

    for u in range(U1):
        give1(u).start()

    def pair1(u):
        m, cs = cut1(u)
        give1(u).wait_recv()
        return part_ref[rows_of(core, m), cs].astype(f32) + d1[m, :, cs].astype(f32)

    def mid_add1(u):
        m, cs = cut1(u)
        pair = pair1(u)
        line1(u).wait_recv()
        t1[m, :, cs] = (pair + l1[m, :, cs].astype(f32)).astype(bf16)
        cross1(u).start()

    def mid_total1(u):
        m, cs = cut1(u)
        cross1(u).wait_recv()
        total = (t1[m, :, cs].astype(f32) + c1[m, :, cs].astype(f32)).astype(bf16)
        x1[m, :, cs] = (res_ref[rows_of(core, m), cs].astype(f32) + total.astype(f32)).astype(bf16)
        if u % CSPLIT == CSPLIT - 1:
            blk = x1[m].astype(f32)
            mean = jnp.mean(blk, axis=-1, keepdims=True)
            cent = blk - mean
            var = jnp.mean(cent * cent, axis=-1, keepdims=True)
            nrm = cent * lax.rsqrt(var + LN_EPS)
            h2[core, m] = (nrm * gs[0:1, :] + gs[1:2, :]).astype(bf16)
            push_h(m).start()
            share_h(m).start()

    @pl.when(mid)
    def _():
        for s in range(U1 + SKEW1):
            if s < U1:
                mid_add1(s)
            if s >= SKEW1:
                mid_total1(s - SKEW1)

    @pl.when(edge)
    def _():
        for u in range(U1):
            m, cs = cut1(u)
            t1[m, :, cs] = pair1(u).astype(bf16)
            line1(u).start()
        for m in range(MSG):
            push_h(m).wait_recv()
            share_h(m).start()

    for m in range(MSG):
        share_h(m).wait_recv()

    load_up.wait()
    nb = 384
    hmat = h2[...].reshape(ROWS, COLS)
    for n in range(wup.shape[1] // nb):
        up = jnp.dot(hmat, wup[:, n * nb:(n + 1) * nb], preferred_element_type=f32)
        act[:, n * nb:(n + 1) * nb] = jnp.square(jnp.maximum(up, 0.0)).astype(bf16)
    load_dn.wait()

    def give2(u):
        return send(p2.at[u, other], d2.at[u], sd2.at[u], rd2.at[u], partner)

    def line2(u):
        return send(t2.at[u], l2.at[u], sl2.at[u], rl2.at[u], line)

    def cross2(u):
        return send(t2.at[u], c2.at[u], sl2.at[u], rc2.at[u], cross)

    def share_o(u):
        return send(obuf.at[u, core], obuf.at[u, core], sop.at[u], rop.at[u], partner)

    def push_o(u):
        return send(obuf.at[u, core], obuf.at[u, core], soe.at[u], roe.at[u], line)

    def put_o(u, half):
        return pltpu.make_async_copy(
            obuf.at[u, half],
            out_hbm.at[pl.ds(pl.multiple_of(half * OWN, OWN), OWN), pl.ds(u * CW2, CW2)],
            o_sem.at[u, half])

    def down(u):
        dn = jnp.dot(act[...], wdn[:, u * CW2:(u + 1) * CW2], preferred_element_type=f32)
        p2[u] = dn.astype(bf16).reshape(2, OWN, CW2)
        give2(u).start()

    def pair2(u):
        give2(u).wait_recv()
        return p2[u, core].astype(f32) + d2[u].astype(f32)

    def mid_add2(u):
        pair = pair2(u)
        line2(u).wait_recv()
        t2[u] = (pair + l2[u].astype(f32)).astype(bf16)
        cross2(u).start()

    def mid_total2(u):
        cross2(u).wait_recv()
        total = (t2[u].astype(f32) + c2[u].astype(f32)).astype(bf16)
        own = x1[:, :, u * CW2:(u + 1) * CW2].reshape(OWN, CW2)
        obuf[u, core] = (own.astype(f32) + total.astype(f32)).astype(bf16)
        push_o(u).start()
        share_o(u).start()
        put_o(u, core).start()

    @pl.when(mid)
    def _():
        down(0)
        down(1)
        for s in range(U2 + SKEW2):
            if s + 2 < U2:
                down(s + 2)
            if s < U2:
                mid_add2(s)
            if s >= SKEW2:
                mid_total2(s - SKEW2)

    @pl.when(edge)
    def _():
        down(0)
        down(1)
        for u in range(U2):
            if u + 2 < U2:
                down(u + 2)
            t2[u] = pair2(u).astype(bf16)
            line2(u).start()
        for u in range(U2):
            push_o(u).wait_recv()
            share_o(u).start()
            put_o(u, core).start()

    for u in range(U2):
        share_o(u).wait_recv()
        put_o(u, other).start()

    for u in range(U1):
        give1(u).wait_send()
        line1(u).wait_send()
    for m in range(MSG):
        share_h(m).wait_send()
    for u in range(U2):
        give2(u).wait_send()
        line2(u).wait_send()
        share_o(u).wait_send()
        put_o(u, core).wait()
        put_o(u, other).wait()

    @pl.when(mid)
    def _():
        for m in range(MSG):
            push_h(m).wait_send()
        for u in range(U2):
            push_o(u).wait_send()


def tail_call(part, residual, gain, shift, w_up, w_down):
    bf16 = jnp.bfloat16
    f32 = jnp.float32
    ff = w_up.shape[1]
    vm = pl.BlockSpec(memory_space=pltpu.VMEM)
    hb = pl.BlockSpec(memory_space=pl.ANY)
    dma = pltpu.SemaphoreType.DMA
    return pl.pallas_call(
        tail_kernel,
        name='tail',
        out_shape=jax.ShapeDtypeStruct((ROWS, COLS), bf16),
        in_specs=[vm, vm, vm, vm, hb, hb],
        out_specs=hb,
        scratch_shapes=[
            pltpu.VMEM((COLS, ff), bf16), pltpu.VMEM((ff, COLS), bf16),
            pltpu.VMEM((MSG, MROWS, COLS), bf16), pltpu.VMEM((MSG, MROWS, COLS), bf16),
            pltpu.VMEM((MSG, MROWS, COLS), bf16), pltpu.VMEM((MSG, MROWS, COLS), bf16),
            pltpu.VMEM((MSG, MROWS, COLS), bf16),
            pltpu.VMEM((2, MSG, MROWS, COLS), bf16),
            pltpu.VMEM((ROWS, ff), bf16),
            pltpu.VMEM((U2, 2, OWN, CW2), bf16),
            pltpu.VMEM((U2, OWN, CW2), bf16), pltpu.VMEM((U2, OWN, CW2), bf16),
            pltpu.VMEM((U2, OWN, CW2), bf16), pltpu.VMEM((U2, OWN, CW2), bf16),
            pltpu.VMEM((U2, 2, OWN, CW2), bf16), pltpu.VMEM((2, COLS), f32),
            dma((2,)),
            dma((U1,)), dma((U1,)), dma((U1,)), dma((U1,)), dma((U1,)),
            dma((MSG,)), dma((MSG,)), dma((MSG,)), dma((MSG,)),
            dma((U2,)), dma((U2,)), dma((U2,)), dma((U2,)), dma((U2,)),
            dma((U2,)), dma((U2,)), dma((U2,)), dma((U2,)),
            dma((U2, 2)),
        ],
        compiler_params=pltpu.CompilerParams(collective_id=0, has_side_effects=True, vmem_limit_bytes=50 * 1024 * 1024),
    )(part, residual, gain, shift, w_up, w_down)


HDIM = 128
SEQ = 512
GRP = 32
NGRP = ROWS // GRP
TCH = 128
ROT = 64


def head_kernel(x_hbm, pos_ref, gain_ref, shift_ref, wq_hbm, wk_hbm, wv_hbm, wo_hbm, k_hbm, v_hbm,
                part_ref, knew_ref, vnew_ref,
                xs, hs, wq, wk, wv, wo, kb, vb, qs, ks, vs, ps, cs, qb, gs, ord_v, ord_s, perm, perm_t,
                in_sem, w_sem, k_sem, v_sem):
    f32 = jnp.float32
    bf16 = jnp.bfloat16
    heads = wq_hbm.shape[1] // HDIM

    load_x = pltpu.make_async_copy(x_hbm, xs, in_sem.at[0])
    load_q = pltpu.make_async_copy(wq_hbm, wq, w_sem.at[0])
    load_k = pltpu.make_async_copy(wk_hbm, wk, w_sem.at[1])
    load_v = pltpu.make_async_copy(wv_hbm, wv, w_sem.at[2])
    load_o = pltpu.make_async_copy(wo_hbm, wo, in_sem.at[1])
    move_ord = pltpu.make_async_copy(ord_v, ord_s, in_sem.at[2])
    load_x.start()
    load_q.start()
    load_k.start()
    load_v.start()

    lane = lax.broadcasted_iota(jnp.int32, (ROWS, HDIM), 1)
    sub = lax.broadcasted_iota(jnp.int32, (ROWS, HDIM), 0)
    pos_lane = jnp.broadcast_to(pos_ref[...].astype(f32), (ROWS, ROWS))
    pos_col = jnp.transpose(pos_lane)
    ahead = jnp.logical_or(pos_col > pos_lane, jnp.logical_and(pos_col == pos_lane, sub < lane))
    rank = jnp.sum(jnp.where(ahead, 1.0, 0.0), axis=0, keepdims=True)
    hot = jnp.where(sub.astype(f32) == rank, 1.0, 0.0)
    hot_t = jnp.transpose(hot)
    perm[...] = hot.astype(bf16)
    perm_t[...] = hot_t.astype(bf16)
    order = jnp.sum(hot_t * sub.astype(f32), axis=0, keepdims=True)
    spos = jnp.sum(hot_t * pos_col, axis=0, keepdims=True)
    ord_v[0:1, :] = order.astype(jnp.int32)
    ord_v[1:2, :] = spos.astype(jnp.int32)

    for j in range(COLS // HDIM):
        at = slice(j * HDIM, (j + 1) * HDIM)
        gs[0:1, at] = 1.0 + gain_ref[j:j + 1, :].astype(f32)
        gs[1:2, at] = shift_ref[j:j + 1, :].astype(f32)
    move_ord.start()

    half = ROT // 2
    pair = lax.rem(lane, half).astype(f32)
    inv = jnp.exp(pair * (-2.0 * math.log(ROPE_BASE) / ROT))
    ang = pos_col * inv
    in_rot = lane < ROT
    cos_t = jnp.where(in_rot, jnp.cos(ang), 1.0)
    sin_a = jnp.sin(ang)
    sin_t = jnp.where(in_rot, jnp.where(lane < half, -sin_a, sin_a), 0.0)

    def rotate(v):
        swap = jnp.where(lane < half, pltpu.roll(v, HDIM - half, 1), pltpu.roll(v, half, 1))
        return (v * cos_t + swap * sin_t).astype(bf16)

    def chunks(g):
        return lax.div(ord_s[1, g * GRP], TCH) + 1

    move_ord.wait()
    for g in range(NGRP):
        size = pl.multiple_of(chunks(g) * TCH, TCH)

        def fetch(hbm, buf, sem):
            def one(i, carry):
                slot = g * GRP + i
                src = pl.ds(pl.multiple_of(ord_s[0, slot] * SEQ, SEQ), size)
                dst = pl.ds(pl.multiple_of(slot * SEQ, SEQ), size)
                pltpu.make_async_copy(hbm.at[src], buf.at[dst], sem.at[g]).start()
                return carry
            lax.fori_loop(0, GRP, one, 0, unroll=8)

        fetch(k_hbm, kb, k_sem)
        fetch(v_hbm, vb, v_sem)
    load_o.start()

    load_x.wait()
    rb = 16
    for r in range(ROWS // rb):
        blk = xs[r * rb:(r + 1) * rb, :].astype(f32)
        mean = jnp.mean(blk, axis=-1, keepdims=True)
        cent = blk - mean
        var = jnp.mean(cent * cent, axis=-1, keepdims=True)
        nrm = cent * lax.rsqrt(var + LN_EPS)
        hs[r * rb:(r + 1) * rb, :] = (nrm * gs[0:1, :] + gs[1:2, :]).astype(bf16)

    load_q.wait()
    load_k.wait()
    load_v.wait()
    qp = jnp.dot(hs[...], wq[...], preferred_element_type=f32).astype(bf16).astype(f32)
    kp = jnp.dot(hs[...], wk[...], preferred_element_type=f32).astype(bf16).astype(f32)
    vp = jnp.dot(hs[...], wv[...], preferred_element_type=f32).astype(bf16)
    k_rot = rotate(kp)
    knew_ref[...] = k_rot
    vnew_ref[...] = vp
    for g in range(4):
        at = pl.ds(g, ROWS, stride=4)
        if g < heads:
            turned = rotate(qp[:, g * HDIM:(g + 1) * HDIM])
            qs[at, :] = jnp.dot(perm[...], turned, preferred_element_type=f32)
        else:
            qs[at, :] = jnp.zeros((ROWS, HDIM), f32)
    k_sort = jnp.dot(perm[...], k_rot, preferred_element_type=f32)
    v_sort = jnp.dot(perm[...], vp, preferred_element_type=f32)
    p_sort = jnp.transpose(jnp.broadcast_to(ord_v[1:2, :].astype(f32), (ROWS, ROWS)))
    for g in range(4):
        at = pl.ds(g, ROWS, stride=4)
        ks[at, :] = k_sort
        vs[at, :] = v_sort
        ps[at, :] = p_sort

    scale = 1.0 / math.sqrt(HDIM)
    lane_b = lax.div(lane, 4)
    row_i = lax.div(lax.broadcasted_iota(jnp.int32, (16, HDIM), 0), 4)

    def attend(g, rows, p_row, new_row, span):
        size = GRP * span
        at_all = pl.ds(0, size)
        pltpu.make_async_copy(k_hbm.at[at_all], kb.at[at_all], k_sem.at[g]).wait()

        def tile(buf, i, lo, n):
            return buf[pl.ds(pl.multiple_of((g * GRP + i) * SEQ, SEQ) + lo, n), :]

        part = span // 2
        raw = [jnp.dot(
            jnp.concatenate([tile(kb, i, h * part, part) for i in range(GRP)], axis=1),
            qb[...], preferred_element_type=f32) for h in range(2)]
        step_t = lax.broadcasted_iota(jnp.int32, (span, HDIM), 0)
        is_new = step_t == p_row
        sc = jnp.where(is_new, new_row, jnp.concatenate(raw, axis=0)) * scale
        sc = jnp.where(step_t <= p_row, sc, -jnp.inf)
        top = jnp.max(sc, axis=0, keepdims=True)
        ex = jnp.exp(sc - top)
        pr = ex * (1.0 / jnp.sum(ex, axis=0, keepdims=True))
        p_new = jnp.sum(jnp.where(is_new, pr, 0.0), axis=0, keepdims=True).astype(bf16).astype(f32)
        new_w = jnp.transpose(jnp.broadcast_to(p_new, (HDIM, HDIM)))
        p_t = jnp.transpose(jnp.where(is_new, 0.0, pr)).astype(bf16)
        extra = new_w * vs[rows, :]
        pltpu.make_async_copy(v_hbm.at[at_all], vb.at[at_all], v_sem.at[g]).wait()
        for j in range(GRP // 4):
            at = j * 16
            right = jnp.concatenate([tile(vb, j * 4 + i, 0, span) for i in range(4)], axis=1)
            mix = jnp.dot(p_t[at:at + 16, :], right, preferred_element_type=f32)
            out = extra[at:at + 16, :]
            for i in range(4):
                out = out + jnp.where(row_i == i, mix[:, i * HDIM:(i + 1) * HDIM], 0.0)
            cs[pl.ds(pl.multiple_of(g * (GRP * 4) + at, 16), 16), :] = out

    def group(g, carry):
        rows = pl.ds(pl.multiple_of(g * (GRP * 4), GRP * 4), GRP * 4)
        qg = qs[rows, :]
        q_t = jnp.transpose(qg)
        p_row = jnp.transpose(ps[rows, :])[0:1, :].astype(jnp.int32)
        new_col = jnp.sum(qg * ks[rows, :], axis=-1, keepdims=True)
        new_row = jnp.transpose(jnp.broadcast_to(new_col, (HDIM, HDIM)))[0:1, :]
        for i in range(GRP):
            qb[i * HDIM:(i + 1) * HDIM, :] = jnp.where(lane_b == i, q_t, 0.0).astype(bf16)
        count = chunks(g)
        for n in range(1, SEQ // TCH + 1):
            @pl.when(count == n)
            def _():
                attend(g, rows, p_row, new_row, n * TCH)
        return carry

    lax.fori_loop(0, NGRP, group, 0)

    ctx = jnp.concatenate([cs[pl.ds(g, ROWS, stride=4), :].astype(bf16) for g in range(heads)], axis=1)
    ctx = jnp.dot(perm_t[...], ctx, preferred_element_type=f32).astype(bf16)
    load_o.wait()
    wide = 512
    for n in range(COLS // wide):
        part_ref[:, n * wide:(n + 1) * wide] = jnp.dot(
            ctx, wo[:, n * wide:(n + 1) * wide], preferred_element_type=f32).astype(bf16)


def head_call(residual, positions, gain, shift, w_q, w_k, w_v, w_o, keys, vals):
    bf16 = jnp.bfloat16
    f32 = jnp.float32
    vm = pl.BlockSpec(memory_space=pltpu.VMEM)
    hb = pl.BlockSpec(memory_space=pl.ANY)
    dma = pltpu.SemaphoreType.DMA
    nq = w_q.shape[1]
    return pl.pallas_call(
        head_kernel,
        name='head',
        out_shape=(jax.ShapeDtypeStruct((ROWS, COLS), bf16),
                   jax.ShapeDtypeStruct((ROWS, HDIM), bf16),
                   jax.ShapeDtypeStruct((ROWS, HDIM), bf16)),
        in_specs=[hb, vm, vm, vm, hb, hb, hb, hb, hb, hb],
        out_specs=(vm, vm, vm),
        scratch_shapes=[
            pltpu.VMEM((ROWS, COLS), bf16), pltpu.VMEM((ROWS, COLS), bf16),
            pltpu.VMEM((COLS, nq), bf16), pltpu.VMEM((COLS, HDIM), bf16), pltpu.VMEM((COLS, HDIM), bf16),
            pltpu.VMEM((nq, COLS), bf16),
            pltpu.VMEM((ROWS * SEQ, HDIM), bf16), pltpu.VMEM((ROWS * SEQ, HDIM), bf16),
            pltpu.VMEM((ROWS * 4, HDIM), f32), pltpu.VMEM((ROWS * 4, HDIM), f32),
            pltpu.VMEM((ROWS * 4, HDIM), f32), pltpu.VMEM((ROWS * 4, HDIM), f32),
            pltpu.VMEM((ROWS * 4, HDIM), f32),
            pltpu.VMEM((GRP * HDIM, HDIM), bf16), pltpu.VMEM((2, COLS), f32),
            pltpu.VMEM((8, ROWS), jnp.int32), pltpu.SMEM((8, ROWS), jnp.int32),
            pltpu.VMEM((ROWS, ROWS), bf16), pltpu.VMEM((ROWS, ROWS), bf16),
            dma((3,)), dma((3,)), dma((NGRP,)), dma((NGRP,)),
        ],
        compiler_params=pltpu.CompilerParams(vmem_limit_bytes=58 * 1024 * 1024),
    )(residual, positions, gain, shift, w_q, w_k, w_v, w_o, keys, vals)


def solution(mesh):
    row_spec = P('dp', None)
    whole_spec = P()
    col_spec = P(None, 'tp')
    wrow_spec = P('tp', None)
    cache_spec = P('dp', None, 'tp', None)
    new_spec = P('dp', 'tp', None)
    arg_specs = (row_spec, P('dp'), whole_spec, whole_spec, col_spec, col_spec, col_spec, wrow_spec, whole_spec, whole_spec, col_spec, wrow_spec, cache_spec, cache_spec)

    def local_step(residual, positions, ln1_gain, ln1_shift, w_q, w_k, w_v, w_o, ln2_gain, ln2_shift, w_up, w_down, k_cache, v_cache):
        row_count = residual.shape[0]
        keys = k_cache.reshape(row_count * k_cache.shape[1], k_cache.shape[3])
        vals = v_cache.reshape(row_count * v_cache.shape[1], v_cache.shape[3])
        attn_part, k_rot, v_head = head_call(residual, positions[None, :], ln1_gain.reshape(COLS // 128, 128), ln1_shift.reshape(COLS // 128, 128), w_q, w_k, w_v, w_o, keys, vals)
        layer_out = tail_call(attn_part, residual, ln2_gain.reshape(COLS // 128, 128), ln2_shift.reshape(COLS // 128, 128), w_up, w_down)
        return layer_out, k_rot[:, None, :], v_head[:, None, :]

    return jax.shard_map(local_step, mesh=mesh, in_specs=arg_specs, out_specs=(row_spec, new_spec, new_spec), check_vma=False)
```
